32 devices in a mesh: gy: 8 (over z, core), gx: 4 (over y, x).
Axes of the slice: x: 2, y: 2, z: 4, core: 2. Of those that a mesh axis runs over, the one named last changes fastest.
Arguments:
- mean_util: float32 [32, 64, 128], P(None, 'gy', 'gx'), may hold values from -4 to 4
- observed_shares: float32 [32, 64, 128], P(None, 'gy', 'gx'), may hold values from 0.002 to 0.02
- characteristics: float32 [4, 32, 64, 128], P(None, None, 'gy', 'gx'), may hold values from -2 to 2
- taste_draws: float32 [4, 512], replicated, may hold values from -4 to 4
- taste_scale: float32 [4], replicated, may hold values from 0.3 to 1
- prior_probs: bfloat16 [32, 64, 128, 512], P(None, 'gy', 'gx'), may hold values from 0 to 0.099609375
- spill_rate: float32 [32], replicated, may hold values from 1 to 8
- utility_rate: float32 [32], replicated, may hold values from 0.1 to 0.6
- adjacency: int32 [4, 64, 128], P(None, 'gy', 'gx'), may hold values from 0 to 3
Outputs:
- final_util: float32 [32, 64, 128], P(None, 'gy', 'gx')
- log_shares: float32 [32, 64, 128], P(None, 'gy', 'gx')
- residual_max: float32 [3], replicated
The draws below stay inside these ranges and needn't reach their ends.
All inputs are finite; a program needn't handle non-finite values. Where the reference program divides by a largest or mean magnitude, that divisor is 1e-20 or more.
Results may differ from the reference program's by a relative error of at most 0.0008.
Values may be sent and summed in bfloat16 or wider, within the bound.
No kernel may reach another device: no remote copies, remote signals or barrier semaphores. Data moves between devices by JAX's collectives and lax.ppermute only.
A program may use at most 192 MiB of HBM per device.

```python
import math
import jax
import jax.numpy as jnp
from jax import lax

J = 32
K = 4
R = 512
ITERS = 3
NROWS = 64
NCOLS = 128


def place_ends(values, key, low, top_value):
    index_at = [jax.random.randint(jax.random.fold_in(key, axis), (), 0, length) for axis, length in enumerate(values.shape)]
    longest = values.shape.index(max(values.shape))
    neighbour = index_at[:longest] + [(index_at[longest] + 1) % values.shape[longest]] + index_at[longest + 1:]
    return values.at[tuple(index_at)].set(low).at[tuple(neighbour)].set(top_value)


def block_scale(stream_key, extent, cuts, smallest, largest):
    def one(dim, blocks):
        heights = jax.random.uniform(jax.random.fold_in(jax.random.fold_in(stream_key, 6), dim), (blocks,), jnp.float32, smallest / len(cuts), largest / len(cuts))
        return jnp.repeat(jnp.exp(heights), extent[dim] // blocks).reshape((-1,) + (1,) * (len(extent) - dim - 1))

    gain = one(*cuts[0])
    for cut in cuts[1:]:
        gain = gain * one(*cut)
    return gain


def normal_values(own_key, shape, width, most, pieces=(), held_as=jnp.bfloat16):
    values = width * jax.random.normal(own_key, shape, jnp.float32)
    if pieces:
        values = values * block_scale(own_key, shape, pieces, -0.22, 0.18)
    return jnp.clip(values, -most, most).astype(held_as)


def setup_inputs(seed: int = 0) -> dict:
    splits = jax.random.split(jax.random.key(seed), 10)
    return {
        "mean_util": normal_values(splits[0], (J, NROWS, NCOLS), 1.0, 4.0, ((1, 8), (2, 4)), jnp.float32),
        "observed_shares": jnp.clip(jnp.exp(math.log(0.02) - 2.30258502 * jax.random.uniform(splits[1], (J, NROWS, NCOLS), jnp.float32) ** block_scale(splits[1], (J, NROWS, NCOLS), ((1, 8), (2, 4)), -0.2, 0.2)), 0.002, 0.02),
        "characteristics": normal_values(splits[2], (K, J, NROWS, NCOLS), 0.7, 2.0, ((2, 8), (3, 4)), jnp.float32),
        "taste_draws": normal_values(splits[3], (K, R), 1.0, 4.0, (), jnp.float32),
        "taste_scale": jnp.clip(jnp.exp(jax.random.uniform(splits[4], (K,), jnp.float32, math.log(0.3), math.log(1.0))), 0.3, 1.0),
        "prior_probs": jnp.clip(0.099609375 * jax.random.uniform(splits[5], (J, NROWS, NCOLS, R), jnp.float32) ** block_scale(splits[5], (J, NROWS, NCOLS, R), ((1, 8), (2, 4)), -0.2, 0.2), 0.0, 0.099609375).astype(jnp.bfloat16),
        "spill_rate": jnp.clip(jnp.exp(jax.random.uniform(splits[6], (J,), jnp.float32, math.log(1.0), math.log(8.0))), 1.0, 8.0),
        "utility_rate": jnp.clip(jax.random.uniform(splits[7], (J,), jnp.float32, 0.1, 0.6), 0.1, 0.6),
        "adjacency": place_ends(jax.random.randint(splits[8], (4, NROWS, NCOLS), 0, 4), jax.random.fold_in(splits[8], 1), 0, 3).astype(jnp.int32),
    }


step_level = 0.2
gap_eps = 1e-6


def neighbour_avg(padded, link_weights, inverse):
    north_side = padded[:, :-2, 1:-1]
    south_side = padded[:, 2:, 1:-1]
    west_side = padded[:, 1:-1, :-2]
    east_side = padded[:, 1:-1, 2:]
    summed = link_weights[0] * north_side + link_weights[1] * south_side
    summed = summed + link_weights[2] * west_side + link_weights[3] * east_side
    return summed * inverse


def reference(mean_util, observed_shares, characteristics, taste_draws, taste_scale, prior_probs, spill_rate, utility_rate, adjacency):
    link_weights = adjacency.astype(jnp.float32)
    inverse = 1.0 / jnp.maximum(jnp.sum(link_weights, axis=0), 1.0)
    log_observed = jnp.log(observed_shares)
    scaled_chars = characteristics * taste_scale[:, None, None, None]
    draws_state = (spill_rate[:, None, None, None] * prior_probs).astype(jnp.bfloat16)
    draws_state = jnp.transpose(draws_state, (1, 0, 2, 3))
    worst_list = []
    log_pred = mean_util
    for iteration in range(ITERS):
        util_padded = jnp.pad(mean_util, ((0, 0), (1, 1), (1, 1)))
        base_util = mean_util + utility_rate[:, None, None] * neighbour_avg(util_padded, link_weights, inverse)
        draws_padded = jnp.pad(draws_state, ((1, 1), (0, 0), (1, 1), (0, 0)))

        def one_row(row_index):
            rows_three = lax.dynamic_slice_in_dim(draws_padded, row_index, 3, 0)
            row_weights = lax.dynamic_slice_in_dim(link_weights, row_index, 1, 1)[:, 0][:, :, None]
            row_inverse = lax.dynamic_slice_in_dim(inverse, row_index, 1, 0)[0][:, None]
            north_side = rows_three[0][:, 1:-1]
            south_side = rows_three[2][:, 1:-1]
            west_side = rows_three[1][:, :-2]
            east_side = rows_three[1][:, 2:]
            spill = row_weights[0] * north_side + row_weights[1] * south_side
            spill = (spill + row_weights[2] * west_side + row_weights[3] * east_side) * row_inverse
            row_chars = lax.dynamic_slice_in_dim(scaled_chars, row_index, 1, 2)[:, :, 0]
            taste_part = jnp.einsum('kjc,kr->jcr', row_chars, taste_draws, precision=lax.Precision.HIGHEST)
            row_base = lax.dynamic_slice_in_dim(base_util, row_index, 1, 1)[:, 0]
            utility = row_base[:, :, None] + taste_part + spill
            exponent = jnp.exp(utility)
            denominator = 1.0 + jnp.sum(exponent, axis=0)
            choice_prob = exponent / denominator
            new_state = (spill_rate[:, None, None] * choice_prob).astype(jnp.bfloat16)
            return jnp.mean(choice_prob, axis=-1), new_state

        row_shares, draws_state = lax.map(one_row, jnp.arange(NROWS, dtype=jnp.int32))
        log_pred = jnp.log(jnp.transpose(row_shares, (1, 0, 2)))
        residual = log_observed - log_pred
        worst_gap = jnp.max(jnp.abs(residual))
        step_size = step_level / (worst_gap + gap_eps)
        mean_util = mean_util + step_size * residual
        worst_list.append(worst_gap)
    return mean_util, log_pred, jnp.stack(worst_list)
```

```python
import functools
import math

import jax
import jax.numpy as jnp
from jax import lax
from jax.experimental import pallas as pl
from jax.experimental.pallas import tpu as pltpu
from jax.sharding import PartitionSpec as P

ITERS = 3
step_level = 0.2
gap_eps = 1e-06
LANES = 128
GROUP = 4
F32 = jnp.float32
BF16 = jnp.bfloat16
LOG2E = 1.0 / math.log(2.0)


def rounded(x):
    return lax.reduce_precision(x, 8, 7)


def split_parts(x, count):
    parts = []
    for _ in range(count):
        part = rounded(x)
        parts.append(part.astype(BF16))
        x = x - part
    return parts


def kernel_parts(x, count):
    parts = []
    for _ in range(count):
        part = x.astype(BF16)
        parts.append(part)
        x = x - part.astype(F32)
    return parts


def dot(a, b):
    return jnp.dot(a, b, preferred_element_type=F32)


def step_kernel(dims, first, last, *refs):
    J, TR, TC, R, ND = dims
    M = TR * TC
    LO = LANES - J
    refs = list(refs)
    parity = refs.pop(0)
    spill = refs.pop(0)
    if not first:
        mall, res_in, mh_in = refs[:3]
        refs = refs[3:]
    mean_in, state, hB, hA, hC, hD, Wl, Wc, T4, dsel, cnt, rate, ispill, logobs = refs[:14]
    refs = refs[14:]
    if last:
        mean_out, res_out, log_out, mloc = refs[:4]
        refs = refs[4:]
    else:
        state_out, pB, pA, pC, pD, mean_out, res_out, mh_out, mloc = refs[:9]
        refs = refs[9:]
    E, den, Wcb, W4b, S_ref, sc_ref = refs[:6]
    if not last:
        colf = refs[6]

    rim = []
    for h in (hB, hA, hC, hD):
        rim.append(h[J, :, 0:LANES].astype(F32) + h[J, :, LANES : 2 * LANES].astype(F32))
    rim.append(jnp.zeros((LANES - 2 * (TR + TC), LANES), F32))
    rim = jnp.concatenate(rim, axis=0)
    if first:
        mean = mean_in[...]
        mh = rim
    else:
        step = step_level / (jnp.max(mall[...]) + gap_eps)
        mean = mean_in[...] + step * res_in[...]
        mh = mh_in[...] + step * rim
    mean_out[...] = mean
    if not last:
        mh_out[...] = mh
    acc = jnp.zeros((M, LANES), F32)
    for part in kernel_parts(mean, 3):
        acc = acc + dot(Wl[...], part)
    for part in kernel_parts(mh, 3):
        acc = acc + dot(Wc[...], part)
    scaled = (mean * cnt[...] + rate[...] * acc) * ispill[...]
    b_hi, b_mid = kernel_parts(scaled, 2)
    Wcb[...] = Wc[...] + b_hi
    for g in range(J // GROUP):
        W4b[g] = T4[g] + b_mid
    sc_ref[...] = LOG2E / cnt[...]
    den[...] = jnp.ones_like(den)

    row_id = lax.broadcasted_iota(jnp.int32, (J, R), 0)
    zeros_mid = jnp.zeros((LO - 2 * (TR + TC), R), BF16)

    def pass_one(g, carry):
        for q in range(GROUP):
            j = g * GROUP + q
            onehot = jnp.where(row_id == j, 1.0, 0.0).astype(BF16)
            cd = jnp.concatenate([hC[j].astype(F32), hD[j].astype(F32)], axis=0).astype(BF16)
            rhs = jnp.concatenate([hB[j], hA[j], cd, zeros_mid, onehot, dsel[q], onehot], axis=0)
            lhs = jnp.concatenate([Wcb[...], W4b[g]], axis=1)
            total = dot(Wl[...], state[j]) + dot(lhs, rhs)
            factor = sc_ref[...] * spill[j]
            factor = jnp.concatenate([factor] * (R // LANES), axis=1)
            e = jnp.exp2(total * factor)
            E[j] = e
            den[...] += e
        return carry

    lax.fori_loop(0, J // GROUP, pass_one, 0)
    den[...] = 1.0 / den[...]

    lane = lax.broadcasted_iota(jnp.int32, (TC, LANES), 1)

    def chunk(mc, carry):
        rows = pl.ds(pl.multiple_of(mc * TC, TC), TC)

        def pass_two(g, sums):
            inverse = den[rows, :]
            for q in range(GROUP):
                j = g * GROUP + q
                prob = E[j, rows, :] * inverse
                if not last:
                    state_out[j, rows, :] = prob.astype(BF16)
                    colf[0, j, pl.ds(mc, 1), :] = prob[0:1]
                    colf[1, j, pl.ds(mc, 1), :] = prob[TC - 1 : TC]
                part = prob[:, 0:LANES]
                for b in range(1, R // LANES):
                    part = part + prob[:, b * LANES : (b + 1) * LANES]
                total = jnp.sum(part, axis=1, keepdims=True)
                sums = jnp.where(lane == LO + j, total, sums)
            return sums

        S_ref[rows, :] = lax.fori_loop(0, J // GROUP, pass_two, jnp.zeros((TC, LANES), F32))
        return carry

    lax.fori_loop(0, TR, chunk, 0)

    full_lane = lax.broadcasted_iota(jnp.int32, (M, LANES), 1)
    log_pred = jnp.log(S_ref[...] * (1.0 / R))
    res = jnp.where(full_lane >= LO, logobs[...] - log_pred, 0.0)
    res_out[...] = res
    mloc[...] = jnp.broadcast_to(jnp.max(jnp.abs(res)), (ND, LANES))
    if last:
        log_out[...] = log_pred
        return

    py = parity[0]
    px = parity[1]

    def plane(ref, values):
        hi, mid = kernel_parts(values, 2)
        ref[J, :, 0:LANES] = hi
        ref[J, :, LANES : 2 * LANES] = mid
        ref[J, :, 2 * LANES :] = jnp.zeros((values.shape[0], R - 2 * LANES), BF16)

    for ref, start in ((pB, py * (M - TC)), (pA, (1 - py) * (M - TC))):
        rows = pl.ds(pl.multiple_of(start, TC), TC)
        plane(ref, res_out[rows, :])

        def copy_rows(j, carry, ref=ref, rows=rows):
            ref[j] = state_out[j, rows, :]
            return carry

        lax.fori_loop(0, J, copy_rows, 0)
    west = res_out[pl.ds(0, TR, stride=TC), :]
    east = res_out[pl.ds(TC - 1, TR, stride=TC), :]
    plane(pC, jnp.where(px == 0, east, west))
    plane(pD, jnp.where(px == 0, west, east))

    def copy_cols(j, carry):
        pC[j] = colf[1 - px, j].astype(BF16)
        pD[j] = colf[px, j].astype(BF16)
        return carry

    lax.fori_loop(0, J, copy_cols, 0)


def run_step(dims, first, last, *args):
    J, TR, TC, R, ND = dims
    M = TR * TC
    smem = pl.BlockSpec(memory_space=pltpu.SMEM)
    vmem = pl.BlockSpec(memory_space=pltpu.VMEM)
    table = jax.ShapeDtypeStruct((M, LANES), F32)
    peak = jax.ShapeDtypeStruct((ND, LANES), F32)
    if last:
        out_shape = (table, table, table, peak)
    else:
        row = jax.ShapeDtypeStruct((J + 1, TC, R), BF16)
        col = jax.ShapeDtypeStruct((J + 1, TR, R), BF16)
        halo = jax.ShapeDtypeStruct((LANES, LANES), F32)
        state = jax.ShapeDtypeStruct((J, M, R), BF16)
        out_shape = (state, row, row, col, col, table, table, halo, peak)
    scratch = [
        pltpu.VMEM((J, M, R), F32),
        pltpu.VMEM((M, R), F32),
        pltpu.VMEM((M, LANES), BF16),
        pltpu.VMEM((J // GROUP, M, LANES), BF16),
        pltpu.VMEM((M, LANES), F32),
        pltpu.VMEM((M, LANES), F32),
    ]
    if not last:
        scratch.append(pltpu.VMEM((2, J, TR, R), F32))
    return pl.pallas_call(
        functools.partial(step_kernel, dims, first, last),
        out_shape=out_shape,
        in_specs=[smem, smem] + [vmem] * (len(args) - 2),
        out_specs=tuple(vmem for _ in out_shape),
        scratch_shapes=scratch,
        compiler_params=pltpu.CompilerParams(vmem_limit_bytes=56 * 1024 * 1024),
        name="first_step" if first else ("last_step" if last else "mid_step"),
    )(*args)


def pair_perms(size):
    near = [(i, i ^ 1) for i in range(size) if (i ^ 1) < size]
    far = [(i, i + 1 if i % 2 else i - 1) for i in range(size)]
    far = [(i, k) for i, k in far if 0 <= k < size]
    return near, far


def local(
    mean_util,
    observed_shares,
    characteristics,
    taste_draws,
    taste_scale,
    prior_probs,
    spill_rate,
    utility_rate,
    adjacency,
):
    J, TR, TC = mean_util.shape
    K, R = taste_draws.shape
    M = TR * TC
    LO = LANES - J
    ny, nx = lax.axis_size("gy"), lax.axis_size("gx")
    dims = (J, TR, TC, R, ny * nx)
    py = lax.axis_index("gy") % 2
    px = lax.axis_index("gx") % 2
    near_y, far_y = pair_perms(ny)
    near_x, far_x = pair_perms(nx)

    def exchange(pB, pA, pC, pD):
        return (
            lax.ppermute(pB, "gy", far_y),
            lax.ppermute(pA, "gy", near_y),
            lax.ppermute(pC, "gx", near_x),
            lax.ppermute(pD, "gx", far_x),
        )

    def first_payload(index, axis):
        state = lax.dynamic_index_in_dim(prior_probs, index, axis, keepdims=False)
        mean = lax.dynamic_index_in_dim(mean_util, index, axis, keepdims=False).T
        parts = [jnp.pad(p, ((0, 0), (LO, 0))) for p in split_parts(mean, 2)]
        tail = jnp.zeros((mean.shape[0], R - 2 * LANES), BF16)
        plane = jnp.concatenate(parts + [tail], axis=1)
        return jnp.concatenate([state, plane[None]], axis=0)

    row_b, row_a = py * (TR - 1), (1 - py) * (TR - 1)
    col_c, col_d = (1 - px) * (TC - 1), px * (TC - 1)
    halos = exchange(
        first_payload(row_b, 1), first_payload(row_a, 1), first_payload(col_c, 2), first_payload(col_d, 2)
    )

    def table(x):
        return jnp.pad(x.reshape(J, M).T, ((0, 0), (LO, 0)))

    links = adjacency.astype(F32).reshape(4, M, 1)
    count = jnp.maximum(jnp.sum(links, axis=0), 1.0)
    me = lax.broadcasted_iota(jnp.int32, (M, M), 0)
    other = lax.broadcasted_iota(jnp.int32, (M, M), 1)
    my_col = me % TC
    Wl = (
        jnp.where(other == me - TC, links[0], 0.0)
        + jnp.where(other == me + TC, links[1], 0.0)
        + jnp.where((other == me - 1) & (my_col > 0), links[2], 0.0)
        + jnp.where((other == me + 1) & (my_col < TC - 1), links[3], 0.0)
    ).astype(BF16)
    mrow = lax.broadcasted_iota(jnp.int32, (M, LANES), 0)
    lane = lax.broadcasted_iota(jnp.int32, (M, LANES), 1)
    r, c = mrow // TC, mrow % TC
    north = jnp.where(r == 0, links[0], 0.0)
    south = jnp.where(r == TR - 1, links[1], 0.0)
    west = jnp.where(c == 0, links[2], 0.0)
    east = jnp.where(c == TC - 1, links[3], 0.0)
    Wc = (
        jnp.where(lane == c, jnp.where(py == 1, south, north), 0.0)
        + jnp.where(lane == TC + c, jnp.where(py == 1, north, south), 0.0)
        + jnp.where(lane == 2 * TC + r, jnp.where(px == 1, west, east), 0.0)
        + jnp.where(lane == 2 * TC + TR + r, jnp.where(px == 1, east, west), 0.0)
    ).astype(BF16)
    cnt = jnp.broadcast_to(count, (M, LANES))

    per_rate = taste_scale[None, :] / spill_rate[:, None]
    taste = characteristics.reshape(K, J, M).transpose(2, 1, 0) * per_rate[None] * count[:, :, None]
    c_hi, c_mid, c_lo = split_parts(taste, 3)
    d_hi, d_mid, d_lo = split_parts(taste_draws, 3)
    lefts = (c_hi, c_hi, c_mid, c_hi, c_mid, c_lo)
    rights = (d_hi, d_mid, d_hi, d_lo, d_mid, d_hi)
    width = GROUP * K
    groups = J // GROUP
    lefts = [x.reshape(M, groups, width).transpose(1, 0, 2) for x in lefts]
    T4 = jnp.concatenate(lefts, axis=2)
    T4 = jnp.pad(T4, ((0, 0), (0, 0), (0, LANES - T4.shape[2])))
    eye = jnp.eye(GROUP, dtype=BF16)
    rights = [(eye[:, :, None, None] * x[None, None]).reshape(GROUP, width, R) for x in rights]
    dsel = jnp.concatenate(rights, axis=1)
    dsel = jnp.pad(dsel, ((0, 0), (0, LO - dsel.shape[1]), (0, 0)))

    rate = jnp.pad(utility_rate[None], ((0, 0), (LO, 0)))
    ispill = jnp.pad((1.0 / spill_rate)[None], ((0, 0), (LO, 0)))
    logobs = jnp.pad(jnp.log(observed_shares).reshape(J, M).T, ((0, 0), (LO, 0)))
    parity = jnp.stack([py, px]).astype(jnp.int32)
    fixed = (Wl, Wc, T4, dsel, cnt, rate, ispill, logobs)

    mean = table(mean_util)
    state = prior_probs.reshape(J, M, R)
    peaks = []
    res = rim = None
    for iteration in range(ITERS):
        first, last = iteration == 0, iteration + 1 == ITERS
        moving = () if first else (peaks[-1], res, rim)
        args = (parity, spill_rate) + moving + (mean, state) + halos + fixed
        out = run_step(dims, first, last, *args)
        if last:
            mean, res, log_pred, peak = out
        else:
            state, pB, pA, pC, pD, mean, res, rim, peak = out
            halos = exchange(pB, pA, pC, pD)
        peaks.append(lax.all_to_all(peak, ("gy", "gx"), 0, 0, tiled=True))
    worst = jnp.stack([jnp.max(p) for p in peaks])
    step = step_level / (worst[-1] + gap_eps)

    def untable(x):
        return x[:, LO:].T.reshape(J, TR, TC)

    return untable(mean + step * res), untable(log_pred), worst


def solution(mesh):
    placed = (
        P(None, "gy", "gx"),
        P(None, "gy", "gx"),
        P(None, None, "gy", "gx"),
        P(),
        P(),
        P(None, "gy", "gx", None),
        P(),
        P(),
        P(None, "gy", "gx"),
    )
    return jax.shard_map(
        local,
        mesh=mesh,
        in_specs=placed,
        out_specs=(P(None, "gy", "gx"), P(None, "gy", "gx"), P()),
        check_vma=False,
    )
```

```python
import functools
import math

import jax
import jax.numpy as jnp
from jax import lax
from jax.experimental import pallas as pl
from jax.experimental.pallas import tpu as pltpu
from jax.sharding import PartitionSpec as P

ITERS = 3
step_level = 0.2
gap_eps = 1e-06
LANES = 128
GROUP = 4
PARTS = 3
LEFT = (0, 0, 1, 0, 1, 2)
RIGHT = (0, 1, 0, 2, 1, 0)
F32 = jnp.float32
BF16 = jnp.bfloat16
LOG2E = 1.0 / math.log(2.0)
VMEM = pl.BlockSpec(memory_space=pltpu.VMEM)
SMEM = pl.BlockSpec(memory_space=pltpu.SMEM)
ANY = pl.BlockSpec(memory_space=pl.ANY)


def shape(dims, dtype=F32):
    return jax.ShapeDtypeStruct(dims, dtype)


def call(body, name, args, in_specs, out_shape, scratch=(), mib=8, out_specs=None):
    return pl.pallas_call(
        body,
        out_shape=out_shape,
        in_specs=in_specs,
        out_specs=out_specs or tuple(VMEM for _ in out_shape),
        scratch_shapes=list(scratch),
        compiler_params=pltpu.CompilerParams(vmem_limit_bytes=mib * 1024 * 1024),
        name=name,
    )(*args)


def kernel_parts(x, count):
    parts = []
    for _ in range(count):
        part = x.astype(BF16)
        parts.append(part)
        x = x - part.astype(F32)
    return parts


def dot(a, b):
    return jnp.dot(a, b, preferred_element_type=F32)


def iota(dims, axis):
    return lax.broadcasted_iota(jnp.int32, dims, axis)


def side_columns(x, lo):
    return jnp.concatenate([jnp.zeros((lo, x.shape[1]), F32), x], axis=0).T


def plane(ref, at, values):
    hi, mid = kernel_parts(values, 2)
    width = ref.shape[-1]
    ref[at, :, 0:LANES] = hi
    ref[at, :, LANES : 2 * LANES] = mid
    ref[at, :, 2 * LANES :] = jnp.zeros((values.shape[0], width - 2 * LANES), BF16)


def rows_kernel(dims, parity, mean, prior, pB, pA, sems):
    J, TR, TC, R, ND = dims
    lo = LANES - J
    py = parity[0]
    row_b, row_a = py * (TR - 1), (1 - py) * (TR - 1)
    copies = []
    for n, (ref, row) in enumerate(((pB, row_b), (pA, row_a))):
        copy = pltpu.make_async_copy(prior.at[:, row], ref.at[pl.ds(0, J)], sems.at[n])
        copy.start()
        copies.append(copy)
    north = side_columns(mean[:, 0, :], lo)
    south = side_columns(mean[:, TR - 1, :], lo)
    plane(pB, J, jnp.where(py == 1, south, north))
    plane(pA, J, jnp.where(py == 1, north, south))
    for copy in copies:
        copy.wait()


def prep_kernel(dims, K, *refs):
    J, TR, TC, R, ND = dims
    M = TR * TC
    lo = LANES - J
    (parity, scale_s, spill, rates, mean, shares, chars, draws, links) = refs[:9]
    (Wl, Wc, T4, dsel, cnt, rate, ispill, table, logobs) = refs[9:18]
    taste, a_s = refs[18:]
    py, px = parity[0], parity[1]

    columns = links[...].astype(F32).reshape(4 * TR, TC)
    columns = jnp.concatenate([columns, jnp.zeros((LANES - 4 * TR, TC), F32)], axis=0).T
    for d in range(4):
        for i in range(TR):
            at = d * TR + i
            a_s[d, i * TC : (i + 1) * TC, :] = jnp.broadcast_to(columns[:, at : at + 1], (TC, LANES))
    count = jnp.maximum(a_s[0] + a_s[1] + a_s[2] + a_s[3], 1.0)
    cnt[...] = count

    me = iota((M, LANES), 0)
    lane = iota((M, LANES), 1)
    r, c = me // TC, me % TC
    for b in range(M // LANES):
        other = lane + b * LANES
        w = jnp.where(other == me - TC, a_s[0], 0.0)
        w = w + jnp.where(other == me + TC, a_s[1], 0.0)
        w = w + jnp.where((other == me - 1) & (c > 0), a_s[2], 0.0)
        w = w + jnp.where((other == me + 1) & (c < TC - 1), a_s[3], 0.0)
        Wl[:, b * LANES : (b + 1) * LANES] = w.astype(BF16)
    north = jnp.where(r == 0, a_s[0], 0.0)
    south = jnp.where(r == TR - 1, a_s[1], 0.0)
    west = jnp.where(c == 0, a_s[2], 0.0)
    east = jnp.where(c == TC - 1, a_s[3], 0.0)
    far_row = jnp.where(py == 1, south, north)
    near_row = jnp.where(py == 1, north, south)
    near_col = jnp.where(px == 1, west, east)
    far_col = jnp.where(px == 1, east, west)
    Wc[...] = (
        jnp.where(lane == c, far_row, 0.0)
        + jnp.where(lane == TC + c, near_row, 0.0)
        + jnp.where(lane == 2 * TC + r, near_col, 0.0)
        + jnp.where(lane == 2 * TC + TR + r, far_col, 0.0)
    ).astype(BF16)
    inverse = 1.0 / spill[...]
    left = jnp.zeros((1, lo), F32)
    rate[...] = jnp.concatenate([left, rates[...]], axis=1)
    ispill[...] = jnp.concatenate([left, inverse], axis=1)
    per_rate = jnp.concatenate([inverse * scale_s[k] for k in range(K)], axis=1)
    for i in range(TR):
        at = slice(i * TC, (i + 1) * TC)
        table[at] = side_columns(mean[:, i, :], lo)
        logobs[at] = side_columns(jnp.log(shares[:, i, :]), lo)
        block = jnp.concatenate([chars[k, :, i, :] for k in range(K)], axis=0).T
        taste[at] = block * per_rate
    parts = kernel_parts(taste[...] * count, PARTS)
    width = GROUP * K
    src = iota((LANES, LANES), 0)
    dst = iota((LANES, LANES), 1)
    term, inner = dst // width, dst % width
    for g in range(J // GROUP):
        wanted = (inner // GROUP) * J + g * GROUP + inner % GROUP
        hit = (src == wanted) & (term < len(LEFT))
        total = jnp.zeros((M, LANES), F32)
        for p in range(PARTS):
            which = functools.reduce(jnp.logical_or, [term == t for t, l in enumerate(LEFT) if l == p])
            total = total + dot(parts[p], jnp.where(hit & which, 1.0, 0.0).astype(BF16))
        T4[g] = total.astype(BF16)

    d_parts = kernel_parts(draws[...], PARTS)
    held = jnp.concatenate([p.astype(F32) for p in d_parts], axis=0)
    held = jnp.concatenate([held, jnp.zeros((LANES - PARTS * K, R), F32)], axis=0).astype(BF16)
    src = iota((LANES, LANES), 1)
    dst = iota((LANES, LANES), 0)
    term, inner = dst // width, dst % width
    for q in range(GROUP):
        hit = jnp.zeros((LANES, LANES), jnp.bool_)
        for t, p in enumerate(RIGHT):
            hit = hit | ((term == t) & (src == p * K + inner // GROUP))
        hit = hit & (inner % GROUP == q)
        dsel[q] = dot(jnp.where(hit, 1.0, 0.0).astype(BF16), held).astype(BF16)


def columns_kernel(dims, parity, mean, state, pC, pD):
    J, TR, TC, R, ND = dims
    M = TR * TC
    lo = LANES - J
    px = parity[1]
    line = iota((2 * TR, M), 0)
    col = jnp.where(line < TR, (1 - px) * (TC - 1), px * (TC - 1))
    pick = jnp.where(iota((2 * TR, M), 1) == (line % TR) * TC + col, 1.0, 0.0).astype(BF16)

    def body(g, carry):
        for q in range(GROUP):
            j = g * GROUP + q
            found = dot(pick, state[j]).astype(BF16)
            pC[j] = found[:TR]
            pD[j] = found[TR:]
        return carry

    lax.fori_loop(0, J // GROUP, body, 0)
    west, east = [], []
    for i in range(TR):
        block = side_columns(mean[:, i, :], lo)
        west.append(block[0:1])
        east.append(block[TC - 1 : TC])
    west = jnp.concatenate(west, axis=0)
    east = jnp.concatenate(east, axis=0)
    plane(pC, J, jnp.where(px == 0, east, west))
    plane(pD, J, jnp.where(px == 0, west, east))


def step_kernel(dims, first, last, *refs):
    J, TR, TC, R, ND = dims
    M = TR * TC
    lo = LANES - J
    refs = list(refs)
    parity = refs.pop(0)
    spill = refs.pop(0)
    if not first:
        mall, res_in, mh_in = refs[:3]
        refs = refs[3:]
    mean_in, state, hB, hA, hC, hD, Wl, Wc, T4, dsel, cnt, rate, ispill, logobs = refs[:14]
    refs = refs[14:]
    if last:
        mean_out, res_out, log_out, mloc = refs[:4]
        refs = refs[4:]
    else:
        state_out, pB, pA, pC, pD, mean_out, res_out, mh_out, mloc = refs[:9]
        refs = refs[9:]
    E, den, Wcb, W4b, S_ref, sc_ref = refs[:6]
    if not last:
        colf = refs[6]

    rim = []
    for h in (hB, hA, hC, hD):
        rim.append(h[J, :, 0:LANES].astype(F32) + h[J, :, LANES : 2 * LANES].astype(F32))
    rim.append(jnp.zeros((LANES - 2 * (TR + TC), LANES), F32))
    rim = jnp.concatenate(rim, axis=0)
    if first:
        mean = mean_in[...]
        mh = rim
    else:
        step = step_level / (jnp.max(mall[...]) + gap_eps)
        mean = mean_in[...] + step * res_in[...]
        mh = mh_in[...] + step * rim
    mean_out[...] = mean
    if not last:
        mh_out[...] = mh
    acc = jnp.zeros((M, LANES), F32)
    for part in kernel_parts(mean, 3):
        acc = acc + dot(Wl[...], part)
    for part in kernel_parts(mh, 3):
        acc = acc + dot(Wc[...], part)
    scaled = (mean * cnt[...] + rate[...] * acc) * ispill[...]
    b_hi, b_mid = kernel_parts(scaled, 2)
    Wcb[...] = Wc[...] + b_hi
    for g in range(J // GROUP):
        W4b[g] = T4[g] + b_mid
    sc_ref[...] = LOG2E / cnt[...]
    den[...] = jnp.ones_like(den)

    row_id = iota((J, R), 0)
    zeros_mid = jnp.zeros((lo - 2 * (TR + TC), R), BF16)

    def pass_one(g, carry):
        for q in range(GROUP):
            j = g * GROUP + q
            onehot = jnp.where(row_id == j, 1.0, 0.0).astype(BF16)
            cd = jnp.concatenate([hC[j].astype(F32), hD[j].astype(F32)], axis=0).astype(BF16)
            rhs = jnp.concatenate([hB[j], hA[j], cd, zeros_mid, onehot, dsel[q, :lo, :], onehot], axis=0)
            lhs = jnp.concatenate([Wcb[...], W4b[g]], axis=1)
            total = dot(Wl[...], state[j]) + dot(lhs, rhs)
            factor = sc_ref[...] * spill[j]
            factor = jnp.concatenate([factor] * (R // LANES), axis=1)
            e = jnp.exp2(total * factor)
            E[j] = e
            den[...] += e
        return carry

    lax.fori_loop(0, J // GROUP, pass_one, 0)

    lane = iota((TC, LANES), 1)

    def chunk(row, carry):
        rows = pl.ds(pl.multiple_of(row * TC, TC), TC)
        inverse = 1.0 / den[rows, :]
        sums = jnp.zeros((TC, LANES), F32)
        for j in range(J):
            prob = E[j, rows, :] * inverse
            if not last:
                state_out[j, rows, :] = prob.astype(BF16)
                colf[0, j, pl.ds(row, 1), :] = prob[0:1]
                colf[1, j, pl.ds(row, 1), :] = prob[TC - 1 : TC]
            part = prob[:, 0:LANES]
            for b in range(1, R // LANES):
                part = part + prob[:, b * LANES : (b + 1) * LANES]
            sums = jnp.where(lane == lo + j, jnp.sum(part, axis=1, keepdims=True), sums)
        S_ref[rows, :] = sums
        return carry

    lax.fori_loop(0, TR, chunk, 0)

    log_pred = jnp.log(S_ref[...] * (1.0 / R))
    res = jnp.where(iota((M, LANES), 1) >= lo, logobs[...] - log_pred, 0.0)
    res_out[...] = res
    mloc[...] = jnp.broadcast_to(jnp.max(jnp.abs(res)), (ND, LANES))
    if last:
        log_out[...] = log_pred
        return

    py = parity[0]
    px = parity[1]
    for ref, start in ((pB, py * (M - TC)), (pA, (1 - py) * (M - TC))):
        rows = pl.ds(pl.multiple_of(start, TC), TC)
        plane(ref, J, res_out[rows, :])

        def copy_rows(j, carry, ref=ref, rows=rows):
            ref[j] = state_out[j, rows, :]
            return carry

        lax.fori_loop(0, J, copy_rows, 0, unroll=4)
    west = res_out[pl.ds(0, TR, stride=TC), :]
    east = res_out[pl.ds(TC - 1, TR, stride=TC), :]
    plane(pC, J, jnp.where(px == 0, east, west))
    plane(pD, J, jnp.where(px == 0, west, east))

    def copy_cols(j, carry):
        pC[j] = colf[1 - px, j].astype(BF16)
        pD[j] = colf[px, j].astype(BF16)
        return carry

    lax.fori_loop(0, J, copy_cols, 0, unroll=4)


def layout_kernel(dims, mean, res, log_pred, mean_t, res_t, log_t):
    J, TR, TC, R, ND = dims
    lo = LANES - J
    for ref, out in ((mean, mean_t), (res, res_t), (log_pred, log_t)):
        for i in range(TR):
            out[:, i, :] = ref[i * TC : (i + 1) * TC, :].T[lo:]


def final_kernel(*refs):
    peaks = refs[:ITERS]
    mean_t, res_t, final, worst = refs[ITERS:]
    for n, peak in enumerate(peaks):
        worst[n] = jnp.max(peak[...])
    step = step_level / (jnp.max(peaks[-1][...]) + gap_eps)
    final[...] = mean_t[...] + step * res_t[...]


def pair_perms(size):
    near = [(i, i ^ 1) for i in range(size) if (i ^ 1) < size]
    far = [(i, i + 1 if i % 2 else i - 1) for i in range(size)]
    far = [(i, k) for i, k in far if 0 <= k < size]
    return near, far


def local(
    mean_util,
    observed_shares,
    characteristics,
    taste_draws,
    taste_scale,
    prior_probs,
    spill_rate,
    utility_rate,
    adjacency,
):
    J, TR, TC = mean_util.shape
    K, R = taste_draws.shape
    M = TR * TC
    lo = LANES - J
    ny, nx = lax.axis_size("gy"), lax.axis_size("gx")
    dims = (J, TR, TC, R, ny * nx)
    py = lax.axis_index("gy") % 2
    px = lax.axis_index("gx") % 2
    parity = jnp.stack([py, px]).astype(jnp.int32)
    near_y, far_y = pair_perms(ny)
    near_x, far_x = pair_perms(nx)

    table = shape((M, LANES))
    row = shape((J + 1, TC, R), BF16)
    col = shape((J + 1, TR, R), BF16)
    peak_shape = shape((ny * nx, LANES))
    cube = shape((J, TR, TC))

    pB, pA = call(
        functools.partial(rows_kernel, dims),
        "rows",
        (parity, mean_util, pltpu.with_memory_space_constraint(prior_probs, pltpu.HBM)),
        [SMEM, VMEM, ANY],
        (row, row),
        [pltpu.SemaphoreType.DMA((2,))],
    )

    def exchange(pB, pA, pC, pD):
        return (
            lax.ppermute(pB, "gy", far_y),
            lax.ppermute(pA, "gy", near_y),
            lax.ppermute(pC, "gx", near_x),
            lax.ppermute(pD, "gx", far_x),
        )

    pC, pD = call(
        functools.partial(columns_kernel, dims),
        "columns",
        (parity, mean_util, prior_probs.reshape(J, M, R)),
        [SMEM, VMEM, VMEM],
        (col, col),
    )
    halos = exchange(pB, pA, pC, pD)

    Wl, Wc, T4, dsel, cnt, rate, ispill, mean, logobs = call(
        functools.partial(prep_kernel, dims, K),
        "prep",
        (
            parity,
            taste_scale,
            spill_rate.reshape(1, J),
            utility_rate.reshape(1, J),
            mean_util,
            observed_shares,
            characteristics,
            taste_draws,
            adjacency,
        ),
        [SMEM, SMEM] + [VMEM] * 7,
        (
            shape((M, M), BF16),
            shape((M, LANES), BF16),
            shape((J // GROUP, M, LANES), BF16),
            shape((GROUP, LANES, R), BF16),
            table,
            shape((1, LANES)),
            shape((1, LANES)),
            table,
            table,
        ),
        [pltpu.VMEM((M, LANES), F32), pltpu.VMEM((4, M, LANES), F32)],
    )

    state = prior_probs.reshape(J, M, R)
    peaks = []
    res = rim = None
    for iteration in range(ITERS):
        first, last = iteration == 0, iteration + 1 == ITERS
        moving = () if first else (peaks[-1], res, rim)
        args = (parity, spill_rate) + moving + (mean, state) + halos
        args = args + (Wl, Wc, T4, dsel, cnt, rate, ispill, logobs)
        if last:
            outs = (table, table, table, peak_shape)
        else:
            outs = (shape((J, M, R), BF16), row, row, col, col, table, table, shape((LANES, LANES)), peak_shape)
        scratch = [
            pltpu.VMEM((J, M, R), F32),
            pltpu.VMEM((M, R), F32),
            pltpu.VMEM((M, LANES), BF16),
            pltpu.VMEM((J // GROUP, M, LANES), BF16),
            pltpu.VMEM((M, LANES), F32),
            pltpu.VMEM((M, LANES), F32),
        ]
        if not last:
            scratch.append(pltpu.VMEM((2, J, TR, R), F32))
        out = call(
            functools.partial(step_kernel, dims, first, last),
            "step",
            args,
            [SMEM, SMEM] + [VMEM] * (len(args) - 2),
            outs,
            scratch,
            mib=23,
        )
        if last:
            mean, res, log_pred, peak = out
        else:
            state, pB, pA, pC, pD, mean, res, rim, peak = out
            halos = exchange(pB, pA, pC, pD)
        peaks.append(lax.all_to_all(peak, ("gy", "gx"), 0, 0, tiled=True))

    mean_t, res_t, log_t = call(
        functools.partial(layout_kernel, dims), "layout", (mean, res, log_pred), [VMEM] * 3, (cube, cube, cube)
    )
    final, worst = call(
        final_kernel,
        "final",
        tuple(peaks) + (mean_t, res_t),
        [VMEM] * (ITERS + 2),
        (cube, shape((ITERS,))),
        out_specs=(VMEM, SMEM),
    )
    return final, log_t, worst


def solution(mesh):
    placed = (
        P(None, "gy", "gx"),
        P(None, "gy", "gx"),
        P(None, None, "gy", "gx"),
        P(),
        P(),
        P(None, "gy", "gx", None),
        P(),
        P(),
        P(None, "gy", "gx"),
    )
    return jax.shard_map(
        local,
        mesh=mesh,
        in_specs=placed,
        out_specs=(P(None, "gy", "gx"), P(None, "gy", "gx"), P()),
        check_vma=False,
    )
```

```python
import functools
import math

import jax
import jax.numpy as jnp
from jax import lax
from jax.experimental import pallas as pl
from jax.experimental.pallas import tpu as pltpu
from jax.sharding import PartitionSpec as P

ITERS = 3
step_level = 0.2
gap_eps = 1e-06
LANES = 128
GROUP = 2
UNROLL = 4
PARTS = 2
LEFT = (0, 0, 1)
RIGHT = (0, 1, 0)
F32 = jnp.float32
BF16 = jnp.bfloat16
LOG2E = 1.0 / math.log(2.0)
VMEM = pl.BlockSpec(memory_space=pltpu.VMEM)
SMEM = pl.BlockSpec(memory_space=pltpu.SMEM)
ANY = pl.BlockSpec(memory_space=pl.ANY)


def shape(dims, dtype=F32):
    return jax.ShapeDtypeStruct(dims, dtype)


def call(body, name, args, in_specs, out_shape, scratch=(), mib=8, out_specs=None, alias=None):
    return pl.pallas_call(
        body,
        out_shape=out_shape,
        in_specs=in_specs,
        out_specs=out_specs or tuple(VMEM for _ in out_shape),
        scratch_shapes=list(scratch),
        input_output_aliases=alias or {},
        compiler_params=pltpu.CompilerParams(vmem_limit_bytes=mib * 1024 * 1024),
        name=name,
    )(*args)


def kernel_parts(x, count):
    parts = []
    for _ in range(count):
        part = x.astype(BF16)
        parts.append(part)
        x = x - part.astype(F32)
    return parts


def dot(a, b):
    return jnp.dot(a, b, preferred_element_type=F32)


def iota(dims, axis):
    return lax.broadcasted_iota(jnp.int32, dims, axis)


def plan(dims, K):
    J, TR, TC, R, ND = dims
    rim = TC
    cols = rim + TC
    taste = cols + 2 * TR
    base = taste + len(LEFT) * GROUP * K
    assert TR * TC == 2 * LANES and base + 2 * GROUP <= LANES
    return rim, cols, taste, base


def side_columns(x, lo):
    return jnp.concatenate([jnp.zeros((lo, x.shape[1]), F32), x], axis=0).T


def plane(ref, at, values):
    hi, mid = kernel_parts(values, 2)
    width = ref.shape[-1]
    ref[at, :, 0:LANES] = hi
    ref[at, :, LANES : 2 * LANES] = mid
    ref[at, :, 2 * LANES :] = jnp.zeros((values.shape[0], width - 2 * LANES), BF16)


def rows_kernel(dims, parity, mean, prior, pB, pA, sems):
    J, TR, TC, R, ND = dims
    lo = LANES - J
    py = parity[0]
    row_b, row_a = py * (TR - 1), (1 - py) * (TR - 1)
    copies = []
    for n, (ref, row) in enumerate(((pB, row_b), (pA, row_a))):
        copy = pltpu.make_async_copy(prior.at[:, row], ref.at[pl.ds(0, J)], sems.at[n])
        copy.start()
        copies.append(copy)
    north = side_columns(mean[:, 0, :], lo)
    south = side_columns(mean[:, TR - 1, :], lo)
    plane(pB, J, jnp.where(py == 1, south, north))
    plane(pA, J, jnp.where(py == 1, north, south))
    for copy in copies:
        copy.wait()


def prep_kernel(dims, K, *refs):
    J, TR, TC, R, ND = dims
    M = TR * TC
    lo = LANES - J
    (parity, scale_s, spill, rates, mean, shares, chars, draws, links) = refs[:9]
    (Wl, Wc, Lf, F, dsel, cnt, rate, ispill, table, logobs) = refs[9:19]
    taste, a_s = refs[19:]
    rim_at, cols_at, taste_at, base_at = plan(dims, K)
    py, px = parity[0], parity[1]

    columns = links[...].astype(F32).reshape(4 * TR, TC)
    columns = jnp.concatenate([columns, jnp.zeros((LANES - 4 * TR, TC), F32)], axis=0).T
    for d in range(4):
        for i in range(TR):
            at = d * TR + i
            a_s[d, i * TC : (i + 1) * TC, :] = jnp.broadcast_to(columns[:, at : at + 1], (TC, LANES))
    count = jnp.maximum(a_s[0] + a_s[1] + a_s[2] + a_s[3], 1.0)
    cnt[...] = count

    me = iota((M, LANES), 0)
    lane = iota((M, LANES), 1)
    r, c = me // TC, me % TC

    def inside(other):
        w = jnp.where(other == me - TC, a_s[0], 0.0)
        w = w + jnp.where(other == me + TC, a_s[1], 0.0)
        w = w + jnp.where((other == me - 1) & (c > 0), a_s[2], 0.0)
        return w + jnp.where((other == me + 1) & (c < TC - 1), a_s[3], 0.0)

    for b in range(M // LANES):
        Wl[:, b * LANES : (b + 1) * LANES] = inside(lane + b * LANES).astype(BF16)
    start = jnp.where(me < LANES, 0, LANES - TC)
    Lf[...] = inside(lane + start).astype(BF16)
    fixed = jnp.where(lane < TC, inside(lane + LANES + start), 0.0)
    north = jnp.where(r == 0, a_s[0], 0.0)
    south = jnp.where(r == TR - 1, a_s[1], 0.0)
    west = jnp.where(c == 0, a_s[2], 0.0)
    east = jnp.where(c == TC - 1, a_s[3], 0.0)
    far_row = jnp.where(py == 1, south, north)
    near_row = jnp.where(py == 1, north, south)
    near_col = jnp.where(px == 1, west, east)
    far_col = jnp.where(px == 1, east, west)
    fixed = (
        fixed
        + jnp.where(lane == rim_at + c, north + south, 0.0)
        + jnp.where(lane == cols_at + r, near_col, 0.0)
        + jnp.where(lane == cols_at + TR + r, far_col, 0.0)
    )
    Wc[...] = (
        jnp.where(lane == c, far_row, 0.0)
        + jnp.where(lane == TC + c, near_row, 0.0)
        + jnp.where(lane == 2 * TC + r, near_col, 0.0)
        + jnp.where(lane == 2 * TC + TR + r, far_col, 0.0)
    ).astype(BF16)
    inverse = 1.0 / spill[...]
    left = jnp.zeros((1, lo), F32)
    rate[...] = jnp.concatenate([left, rates[...]], axis=1)
    ispill[...] = jnp.concatenate([left, inverse], axis=1)
    per_rate = jnp.concatenate([inverse * scale_s[k] for k in range(K)], axis=1)
    for i in range(TR):
        at = slice(i * TC, (i + 1) * TC)
        table[at] = side_columns(mean[:, i, :], lo)
        logobs[at] = side_columns(jnp.log(shares[:, i, :]), lo)
        block = jnp.concatenate([chars[k, :, i, :] for k in range(K)], axis=0).T
        taste[at] = block * per_rate
    parts = kernel_parts(taste[...] * count, PARTS)
    width = GROUP * K
    src = iota((LANES, LANES), 0)
    dst = iota((LANES, LANES), 1) - taste_at
    term, inner = dst // width, dst % width
    for g in range(J // GROUP):
        wanted = (inner // GROUP) * J + g * GROUP + inner % GROUP
        hit = (src == wanted) & (dst >= 0) & (dst < base_at - taste_at)
        total = fixed
        for p in range(PARTS):
            which = functools.reduce(jnp.logical_or, [term == t for t, l in enumerate(LEFT) if l == p])
            total = total + dot(parts[p], jnp.where(hit & which, 1.0, 0.0).astype(BF16))
        F[g] = total.astype(BF16)

    d_parts = kernel_parts(draws[...], PARTS)
    held = jnp.concatenate([p.astype(F32) for p in d_parts], axis=0)
    held = jnp.concatenate([held, jnp.zeros((LANES - PARTS * K, R), F32)], axis=0).astype(BF16)
    deep = LANES - taste_at
    src = iota((deep, LANES), 1)
    dst = iota((deep, LANES), 0)
    term, inner = dst // width, dst % width
    line = iota((deep, R), 0) - (base_at - taste_at)
    for q in range(GROUP):
        hit = jnp.zeros((deep, LANES), jnp.bool_)
        for t, p in enumerate(RIGHT):
            hit = hit | ((term == t) & (src == p * K + inner // GROUP))
        hit = hit & (inner % GROUP == q)
        ones = jnp.where((line == q) | (line == GROUP + q), 1.0, 0.0)
        dsel[q] = (dot(jnp.where(hit, 1.0, 0.0).astype(BF16), held) + ones).astype(BF16)


def columns_kernel(dims, parity, mean, state, pC, pD):
    J, TR, TC, R, ND = dims
    M = TR * TC
    lo = LANES - J
    px = parity[1]
    line = iota((2 * TR, M), 0)
    col = jnp.where(line < TR, (1 - px) * (TC - 1), px * (TC - 1))
    pick = jnp.where(iota((2 * TR, M), 1) == (line % TR) * TC + col, 1.0, 0.0).astype(BF16)

    for j in range(J):
        found = dot(pick, state[j]).astype(BF16)
        pC[j] = found[:TR]
        pD[j] = found[TR:]
    west, east = [], []
    for i in range(TR):
        block = side_columns(mean[:, i, :], lo)
        west.append(block[0:1])
        east.append(block[TC - 1 : TC])
    west = jnp.concatenate(west, axis=0)
    east = jnp.concatenate(east, axis=0)
    plane(pC, J, jnp.where(px == 0, east, west))
    plane(pD, J, jnp.where(px == 0, west, east))


def step_kernel(dims, K, first, last, *refs):
    J, TR, TC, R, ND = dims
    M = TR * TC
    lo = LANES - J
    refs = list(refs)
    parity = refs.pop(0)
    spill = refs.pop(0)
    if not first:
        mall, res_in, mh_in = refs[:3]
        refs = refs[3:]
    mean_in, state, hB, hA, hC, hD, Wl, Wc, Lf, F, dsel, cnt, rate, ispill, logobs = refs[:15]
    refs = refs[15:]
    if last:
        mean_out, res_out, log_out, mloc = refs[:4]
        refs = refs[4:]
    else:
        state_out, pB, pA, pC, pD, mean_out, res_out, mh_out, mloc = refs[:9]
        refs = refs[9:]
    E, den, W, S_ref, sc_ref = refs[:5]
    if not last:
        colf = refs[5]

    rim = []
    for h in (hB, hA, hC, hD):
        rim.append(h[J, :, 0:LANES].astype(F32) + h[J, :, LANES : 2 * LANES].astype(F32))
    rim.append(jnp.zeros((LANES - 2 * (TR + TC), LANES), F32))
    rim = jnp.concatenate(rim, axis=0)
    if first:
        mean = mean_in[...]
        mh = rim
    else:
        step = step_level / (jnp.max(mall[...]) + gap_eps)
        mean = mean_in[...] + step * res_in[...]
        mh = mh_in[...] + step * rim
    mean_out[...] = mean
    if not last:
        mh_out[...] = mh
    acc = jnp.zeros((M, LANES), F32)
    for part in kernel_parts(mean, 3):
        acc = acc + dot(Wl[...], part)
    for part in kernel_parts(mh, 3):
        acc = acc + dot(Wc[...], part)
    scaled = (mean * cnt[...] + rate[...] * acc) * ispill[...]
    b_hi, b_mid = kernel_parts(scaled, 2)
    src = iota((LANES, LANES), 0) - lo
    dst = iota((LANES, LANES), 1)
    spot = 2 * GROUP * (src // GROUP) + src % GROUP
    hi_to = jnp.where((src >= 0) & (dst == spot), 1.0, 0.0).astype(BF16)
    mid_to = jnp.where((src >= 0) & (dst == spot + GROUP), 1.0, 0.0).astype(BF16)
    mixed = dot(b_hi, hi_to) + dot(b_mid, mid_to)
    base_at = plan(dims, K)[3]
    full_lane = iota((M, LANES), 1)
    in_base = (full_lane >= base_at) & (full_lane < base_at + 2 * GROUP)
    for g in range(J // GROUP):
        moved = pltpu.roll(mixed, (base_at - 2 * GROUP * g) % LANES, axis=1)
        W[g] = F[g] + jnp.where(in_base, moved, 0.0).astype(BF16)
    sc_ref[...] = LOG2E / cnt[...]
    den[...] = jnp.ones_like(den)

    odd = parity[0] == 1
    span = LANES + TC

    def pass_one(trip, carry):
        for n in range(UNROLL):
            g = trip * UNROLL + n
            for q in range(GROUP):
                j = g * GROUP + q
                cd = jnp.concatenate([hC[j].astype(F32), hD[j].astype(F32)], axis=0).astype(BF16)
                far, close = hB[j], hA[j]
                rims = (jnp.where(odd, close, far), jnp.where(odd, far, close))
                for b in range(2):
                    rows = slice(b * LANES, (b + 1) * LANES)
                    local_rows = state[j, b * (M - span) : b * (M - span) + span, :]
                    rhs = jnp.concatenate([local_rows, rims[b], cd, dsel[q]], axis=0)
                    lhs = jnp.concatenate([Lf[rows, :], W[g, rows, :]], axis=1)
                    factor = sc_ref[rows, :] * spill[j]
                    factor = jnp.concatenate([factor] * (R // LANES), axis=1)
                    e = jnp.exp2(dot(lhs, rhs) * factor)
                    E[j, rows, :] = e
                    den[rows, :] += e
        return carry

    lax.fori_loop(0, J // (GROUP * UNROLL), pass_one, 0)

    lane = iota((TC, LANES), 1)

    def chunk(row, carry):
        rows = pl.ds(pl.multiple_of(row * TC, TC), TC)
        inverse = 1.0 / den[rows, :]
        sums = jnp.zeros((TC, LANES), F32)
        for j in range(J):
            prob = E[j, rows, :] * inverse
            if not last:
                state_out[j, rows, :] = prob.astype(BF16)
                colf[0, j, pl.ds(row, 1), :] = prob[0:1]
                colf[1, j, pl.ds(row, 1), :] = prob[TC - 1 : TC]
            part = prob[:, 0:LANES]
            for b in range(1, R // LANES):
                part = part + prob[:, b * LANES : (b + 1) * LANES]
            sums = jnp.where(lane == lo + j, jnp.sum(part, axis=1, keepdims=True), sums)
        S_ref[rows, :] = sums
        return carry

    lax.fori_loop(0, TR, chunk, 0)

    log_pred = jnp.log(S_ref[...] * (1.0 / R))
    res = jnp.where(iota((M, LANES), 1) >= lo, logobs[...] - log_pred, 0.0)
    res_out[...] = res
    mloc[...] = jnp.broadcast_to(jnp.max(jnp.abs(res)), (ND, LANES))
    if last:
        log_out[...] = log_pred
        return

    py = parity[0]
    px = parity[1]
    for ref, start in ((pB, py * (M - TC)), (pA, (1 - py) * (M - TC))):
        rows = pl.ds(pl.multiple_of(start, TC), TC)
        plane(ref, J, res_out[rows, :])

        def copy_rows(j, carry, ref=ref, rows=rows):
            ref[j] = state_out[j, rows, :]
            return carry

        lax.fori_loop(0, J, copy_rows, 0, unroll=4)
    west = res_out[pl.ds(0, TR, stride=TC), :]
    east = res_out[pl.ds(TC - 1, TR, stride=TC), :]
    plane(pC, J, jnp.where(px == 0, east, west))
    plane(pD, J, jnp.where(px == 0, west, east))

    def copy_cols(j, carry):
        pC[j] = colf[1 - px, j].astype(BF16)
        pD[j] = colf[px, j].astype(BF16)
        return carry

    lax.fori_loop(0, J, copy_cols, 0, unroll=4)


def layout_kernel(dims, mean, res, log_pred, mean_t, res_t, log_t):
    J, TR, TC, R, ND = dims
    lo = LANES - J
    for ref, out in ((mean, mean_t), (res, res_t), (log_pred, log_t)):
        for i in range(TR):
            out[:, i, :] = ref[i * TC : (i + 1) * TC, :].T[lo:]


def final_kernel(*refs):
    peaks = refs[:ITERS]
    mean_t, res_t, final, worst = refs[ITERS:]
    for n, peak in enumerate(peaks):
        worst[n] = jnp.max(peak[...])
    step = step_level / (jnp.max(peaks[-1][...]) + gap_eps)
    final[...] = mean_t[...] + step * res_t[...]


def pair_perms(size):
    near = [(i, i ^ 1) for i in range(size) if (i ^ 1) < size]
    far = [(i, i + 1 if i % 2 else i - 1) for i in range(size)]
    far = [(i, k) for i, k in far if 0 <= k < size]
    return near, far


def local(
    mean_util,
    observed_shares,
    characteristics,
    taste_draws,
    taste_scale,
    prior_probs,
    spill_rate,
    utility_rate,
    adjacency,
):
    J, TR, TC = mean_util.shape
    K, R = taste_draws.shape
    M = TR * TC
    lo = LANES - J
    ny, nx = lax.axis_size("gy"), lax.axis_size("gx")
    dims = (J, TR, TC, R, ny * nx)
    py = lax.axis_index("gy") % 2
    px = lax.axis_index("gx") % 2
    parity = jnp.stack([py, px]).astype(jnp.int32)
    near_y, far_y = pair_perms(ny)
    near_x, far_x = pair_perms(nx)

    table = shape((M, LANES))
    row = shape((J + 1, TC, R), BF16)
    col = shape((J + 1, TR, R), BF16)
    peak_shape = shape((ny * nx, LANES))
    cube = shape((J, TR, TC))

    pB, pA = call(
        functools.partial(rows_kernel, dims),
        "rows",
        (parity, mean_util, pltpu.with_memory_space_constraint(prior_probs, pltpu.HBM)),
        [SMEM, VMEM, ANY],
        (row, row),
        [pltpu.SemaphoreType.DMA((2,))],
    )

    def exchange(pB, pA, pC, pD):
        return (
            lax.ppermute(pB, "gy", far_y),
            lax.ppermute(pA, "gy", near_y),
            lax.ppermute(pC, "gx", near_x),
            lax.ppermute(pD, "gx", far_x),
        )

    pC, pD = call(
        functools.partial(columns_kernel, dims),
        "columns",
        (parity, mean_util, prior_probs.reshape(J, M, R)),
        [SMEM, VMEM, VMEM],
        (col, col),
    )
    halos = exchange(pB, pA, pC, pD)

    Wl, Wc, Lf, F, dsel, cnt, rate, ispill, mean, logobs = call(
        functools.partial(prep_kernel, dims, K),
        "prep",
        (
            parity,
            taste_scale,
            spill_rate.reshape(1, J),
            utility_rate.reshape(1, J),
            mean_util,
            observed_shares,
            characteristics,
            taste_draws,
            adjacency,
        ),
        [SMEM, SMEM] + [VMEM] * 7,
        (
            shape((M, M), BF16),
            shape((M, LANES), BF16),
            shape((M, LANES), BF16),
            shape((J // GROUP, M, LANES), BF16),
            shape((GROUP, LANES - plan(dims, K)[2], R), BF16),
            table,
            shape((1, LANES)),
            shape((1, LANES)),
            table,
            table,
        ),
        [pltpu.VMEM((M, LANES), F32), pltpu.VMEM((4, M, LANES), F32)],
    )

    state = prior_probs.reshape(J, M, R)
    peaks = []
    res = rim = None
    for iteration in range(ITERS):
        first, last = iteration == 0, iteration + 1 == ITERS
        moving = () if first else (peaks[-1], res, rim)
        args = (parity, spill_rate) + moving + (mean, state) + halos
        args = args + (Wl, Wc, Lf, F, dsel, cnt, rate, ispill, logobs)
        if last:
            outs = (table, table, table, peak_shape)
        else:
            outs = (shape((J, M, R), BF16), row, row, col, col, table, table, shape((LANES, LANES)), peak_shape)
        scratch = [
            pltpu.VMEM((J, M, R), F32),
            pltpu.VMEM((M, R), F32),
            pltpu.VMEM((J // GROUP, M, LANES), BF16),
            pltpu.VMEM((M, LANES), F32),
            pltpu.VMEM((M, LANES), F32),
        ]
        if not last:
            scratch.append(pltpu.VMEM((2, J, TR, R), F32))
        out = call(
            functools.partial(step_kernel, dims, K, first, last),
            "step",
            args,
            [SMEM, SMEM] + [VMEM] * (len(args) - 2),
            outs,
            scratch,
            mib=22,
            alias={} if first or last else {6: 0},
        )
        if last:
            mean, res, log_pred, peak = out
        else:
            state, pB, pA, pC, pD, mean, res, rim, peak = out
            halos = exchange(pB, pA, pC, pD)
        peaks.append(lax.all_to_all(peak, ("gy", "gx"), 0, 0, tiled=True))

    mean_t, res_t, log_t = call(
        functools.partial(layout_kernel, dims), "layout", (mean, res, log_pred), [VMEM] * 3, (cube, cube, cube)
    )
    final, worst = call(
        final_kernel,
        "final",
        tuple(peaks) + (mean_t, res_t),
        [VMEM] * (ITERS + 2),
        (cube, shape((ITERS,))),
        out_specs=(VMEM, SMEM),
    )
    return final, log_t, worst


def solution(mesh):
    placed = (
        P(None, "gy", "gx"),
        P(None, "gy", "gx"),
        P(None, None, "gy", "gx"),
        P(),
        P(),
        P(None, "gy", "gx", None),
        P(),
        P(),
        P(None, "gy", "gx"),
    )
    return jax.shard_map(
        local,
        mesh=mesh,
        in_specs=placed,
        out_specs=(P(None, "gy", "gx"), P(None, "gy", "gx"), P()),
        check_vma=False,
    )
```
